256 devices in a mesh: seq: 128 (over y, z, x_hi, core), batch: 2 (over x_lo).
Axes of the slice: x: 4 (x_hi: 2, x_lo: 2; x = x_hi * 2 + x_lo), y: 4, z: 8, core: 2. Of those that a mesh axis runs over, the one named last changes fastest.
Arguments:
- stream_in: bfloat16 [320, 2097152], P(None, ('batch', 'seq')), parts along dimension 1, may hold values from -6 to 6
- norm_gains: float32 [2, 320], replicated, may hold values from 0.5 to 1.5
- w_inner: bfloat16 [2, 320, 640], replicated, may hold values from -0.3125 to 0.3125
- w_outer: bfloat16 [2, 640, 320], replicated, may hold values from -0.25 to 0.25
Outputs:
- stream_out: bfloat16 [320, 2097152], P(None, ('batch', 'seq')), parts along dimension 1
The draws below stay inside these ranges and needn't reach their ends.
There are 2 independent parts, one for each index of `batch`. The reference program is written for one: setup_inputs(seed, part) draws one part's arguments, and reference() takes and returns one part's arrays. A program takes and returns all parts, laid end to end along the dimension named above; an argument that names none is the same for every part. Nothing has to cross between parts.
All inputs are finite; a program needn't handle non-finite values.
Results may differ from the reference program's by a relative error of at most 0.0059.
Values may be sent and summed in bfloat16 or wider, within the bound.
A program may use at most 64 MiB of HBM per device.

```python
import jax
import jax.numpy as jnp
from jax import lax

TRACKS = 20
TRACK_W = 16
HID = 640
LAYERS = 2
D = 320
LENGTH = 1048576


def block_levels(stream_key, extent, shards, smallest, high):
    def one(axis_at, parts):
        steps = jax.random.uniform(jax.random.fold_in(jax.random.fold_in(stream_key, 6), axis_at), (parts,), jnp.float32, smallest / len(shards), high / len(shards))
        return jnp.repeat(jnp.exp(steps), extent[axis_at] // parts).reshape((-1,) + (1,) * (len(extent) - axis_at - 1))

    level = one(*shards[0])
    for cut in shards[1:]:
        level = level * one(*cut)
    return level


def scatter_about(stream_key, extent, width, most, shards=(), held_as=jnp.bfloat16):
    drawn = width * jax.random.normal(stream_key, extent, jnp.float32)
    if shards:
        drawn = drawn * block_levels(stream_key, extent, shards, -0.22, 0.18)
    return jnp.clip(drawn, -most, most).astype(held_as)


def setup_inputs(seed: int = 0, part: int = 0) -> dict:
    key_list = jax.random.split(jax.random.key(seed), 5)
    own_keys = jax.random.split(jax.random.fold_in(key_list[4], part), 5)
    return {
        "stream_in": scatter_about(own_keys[0], (D, LENGTH), 1.0, 6.0, ((1, 128),)),
        "norm_gains": jnp.clip(1.0 + 0.1 * jax.random.normal(key_list[1], (LAYERS, D), jnp.float32), 0.5, 1.5),
        "w_inner": scatter_about(key_list[2], (LAYERS, D, HID), D ** -0.5, 0.3125),
        "w_outer": scatter_about(key_list[3], (LAYERS, HID, D), HID ** -0.5, 0.25),
    }


def rotate(stream):
    pieces = []
    for track in range(TRACKS):
        offset = 2 ** track % LENGTH
        rows = stream[track * TRACK_W:(track + 1) * TRACK_W, :]
        pieces.append(jnp.roll(rows, offset, axis=1))
    return jnp.concatenate(pieces, axis=0)

def mixer_layer(stream, gain, inner, outer):
    rotated = rotate(stream)
    values = rotated.astype(jnp.float32)
    average = lax.optimization_barrier(jnp.mean(values, axis=0, keepdims=True))
    spread = lax.optimization_barrier(jnp.mean((values - average) ** 2, axis=0, keepdims=True))
    normed = ((values - average) * lax.rsqrt(spread + 1e-05) * gain[:, None]).astype(jnp.bfloat16)
    inner_sum = lax.dot_general(inner, normed, (((0,), (0,)), ((), ())), preferred_element_type=jnp.float32)
    hidden = jax.nn.gelu(inner_sum, approximate=False).astype(jnp.bfloat16)
    outer_sum = lax.dot_general(outer, hidden, (((0,), (0,)), ((), ())), preferred_element_type=jnp.float32)
    return (values + outer_sum).astype(jnp.bfloat16)

def reference(stream_in, norm_gains, w_inner, w_outer):
    stream = stream_in
    for layer_index in range(LAYERS):
        stream = mixer_layer(stream, norm_gains[layer_index], w_inner[layer_index], w_outer[layer_index])
    return stream
```

```python
import functools

import jax
import jax.numpy as jnp
from jax import lax
from jax.experimental import pallas as pl
from jax.experimental.pallas import tpu as pltpu
from jax.sharding import PartitionSpec as P

TRACKS = 20
WIDTH = 16
LAYERS = 2
DIM = 320
HID = 640
RING = 128
COLS = 8192
NEAR = 13
NEAR_ROWS = NEAR * WIDTH
FAR_ROWS = DIM - NEAR_ROWS
PAD = 4096
CHUNKS = 8
CHUNK = COLS // CHUNKS
SUB = 256
LANES = 128
FAR = tuple(2**e for e in range(TRACKS - NEAR))

HALOS = (
    (0, 128, 128, 7),
    (128, 16, 256, 7),
    (144, 16, 512, 7),
    (192, 16, 1024, 4),
    (192, 16, 1024, 5),
    (176, 32, 1024, 6),
    (160, 48, 1024, 7),
)


def halo_slices(index):
    row, rows, cols, chunk = HALOS[index]
    start = (chunk + 1) * CHUNK - cols
    return pl.ds(row, rows), start, cols


def body(
    x_ref, gain_ref, inner_ref, outer_ref, out_ref,
    near, far, made, gains, inner_t, outer_t, inner_raw, outer_raw, rotated, staged,
    local_sem, weight_sem, far_send, far_recv, halo_send, halo_recv, out_sem,
):
    me = lax.axis_index("seq")
    ahead = [lax.rem(me + d, RING) for d in FAR]
    behind = [lax.rem(me + RING - d, RING) for d in FAR]

    near_copy = pltpu.make_async_copy(
        x_ref.at[pl.ds(0, NEAR_ROWS), :], near.at[0, :, pl.ds(PAD, COLS)], local_sem
    )
    near_copy.start()
    inner_copy = pltpu.make_async_copy(inner_ref, inner_raw, weight_sem.at[0])
    outer_copy = pltpu.make_async_copy(outer_ref, outer_raw, weight_sem.at[1])
    inner_copy.start()
    outer_copy.start()

    barrier = pltpu.get_barrier_semaphore()
    for peer in ahead + behind:
        pl.semaphore_signal(barrier, inc=1, device_id={"seq": peer})
    pl.semaphore_wait(barrier, 2 * len(FAR))

    def halo_copy(layer, index, source):
        rows, start, cols = halo_slices(index)
        return pltpu.make_async_remote_copy(
            src_ref=source.at[rows, pl.ds(start + (0 if layer == 0 else PAD), cols)],
            dst_ref=near.at[layer, rows, pl.ds(start + PAD - COLS, cols)],
            send_sem=halo_send.at[layer, index],
            recv_sem=halo_recv.at[layer, index],
            device_id={"seq": ahead[0]},
        )

    def far_copy(layer, track, chunk, source, base):
        cols = pl.ds(pl.multiple_of(chunk * CHUNK, CHUNK), CHUNK)
        return pltpu.make_async_remote_copy(
            src_ref=source.at[pl.ds(base + track * WIDTH, WIDTH), cols],
            dst_ref=far.at[layer, pl.ds(track * WIDTH, WIDTH), cols],
            send_sem=far_send.at[layer],
            recv_sem=far_recv.at[layer, chunk],
            device_id={"seq": ahead[track]},
        )

    def send_far(layer, chunk, source, base):
        for track in range(len(FAR)):
            far_copy(layer, track, chunk, source, base).start()

    for index in range(len(HALOS)):
        halo_copy(0, index, x_ref).start()

    @pl.loop(0, CHUNKS)
    def _(step):
        send_far(0, lax.rem(step + CHUNKS // 2, CHUNKS), x_ref, NEAR_ROWS)

    for layer in range(LAYERS):
        gains[layer] = jnp.broadcast_to(gain_ref[layer : layer + 1, :], (LANES, DIM)).T
    inner_copy.wait()
    for layer in range(LAYERS):
        inner_t[layer] = inner_raw[layer].T
    outer_copy.wait()
    for layer in range(LAYERS):
        outer_t[layer] = outer_raw[layer].T
    near_copy.wait()

    def mix(layer, at, store):
        base = pl.multiple_of(PAD + at, LANES)
        for track in range(NEAR):
            shift = 2**track
            rows = pl.ds(track * WIDTH, WIDTH)
            if shift < LANES:
                wide = near[layer, rows, pl.ds(pl.multiple_of(base - LANES, LANES), SUB + LANES)]
                piece = pltpu.roll(wide.astype(jnp.float32), shift, 1)[:, LANES:]
            else:
                piece = near[layer, rows, pl.ds(pl.multiple_of(base - shift, LANES), SUB)].astype(jnp.float32)
            rotated[rows, :] = piece
        rotated[NEAR_ROWS:, :] = far[layer, :, pl.ds(pl.multiple_of(at, LANES), SUB)].astype(jnp.float32)
        values = rotated[...]
        average = jnp.sum(values, axis=0, keepdims=True) * (1.0 / DIM)
        centred = values - average
        spread = jnp.sum(centred * centred, axis=0, keepdims=True) * (1.0 / DIM)
        scale = lax.rsqrt(spread + 1e-05)
        gain = jnp.concatenate([gains[layer]] * (SUB // LANES), axis=1)
        normed = (centred * scale * gain).astype(jnp.bfloat16)
        inner_sum = jnp.dot(inner_t[layer], normed, preferred_element_type=jnp.float32)
        hidden = (0.5 * inner_sum * (1.0 + lax.erf(inner_sum * (0.5**0.5)))).astype(jnp.bfloat16)
        outer_sum = jnp.dot(outer_t[layer], hidden, preferred_element_type=jnp.float32)
        store((rotated[...] + outer_sum).astype(jnp.bfloat16))

    def wait_far(layer, chunk):
        cols = pl.ds(pl.multiple_of(chunk * CHUNK, CHUNK), CHUNK)
        whole = far.at[layer, :, cols]
        pltpu.make_async_copy(whole, whole, far_recv.at[layer, chunk]).wait()

    def wait_halos(layer, source):
        for index in range(len(HALOS)):
            halo_copy(layer, index, source).wait_recv()

    @pl.loop(0, CHUNKS)
    def _(step):
        chunk = lax.rem(step + CHUNKS // 2, CHUNKS)
        wait_far(0, chunk)

        @pl.when(step == CHUNKS // 2)
        def _():
            wait_halos(0, x_ref)

        @pl.loop(0, CHUNK // SUB)
        def _(part):
            at = pl.multiple_of(chunk * CHUNK + part * SUB, SUB)

            def store(result):
                near[1, :, pl.ds(pl.multiple_of(PAD + at, SUB), SUB)] = result[:NEAR_ROWS]
                made[:, pl.ds(at, SUB)] = result[NEAR_ROWS:]

            mix(0, at, store)

        send_far(1, chunk, made, 0)
        for index, halo in enumerate(HALOS):
            @pl.when(chunk == halo[3])
            def _():
                halo_copy(1, index, near.at[1]).start()

    def out_copy(slot, chunk):
        cols = pl.ds(pl.multiple_of(chunk * CHUNK, CHUNK), CHUNK)
        return pltpu.make_async_copy(staged.at[slot], out_ref.at[:, cols], out_sem.at[slot])

    @pl.loop(0, CHUNKS)
    def _(step):
        chunk = lax.rem(step + CHUNKS // 2, CHUNKS)
        slot = lax.rem(step, 2)
        wait_far(1, chunk)

        @pl.when(step == CHUNKS // 2)
        def _():
            wait_halos(1, near.at[1])

        @pl.when(step >= 2)
        def _():
            out_copy(slot, chunk).wait()

        @pl.loop(0, CHUNK // SUB)
        def _(part):
            at = pl.multiple_of(chunk * CHUNK + part * SUB, SUB)

            def store(result):
                staged[slot, :, pl.ds(pl.multiple_of(part * SUB, SUB), SUB)] = result

            mix(1, at, store)

        out_copy(slot, chunk).start()

    out_copy(0, 0).wait()
    out_copy(1, 0).wait()
    for layer in range(LAYERS):
        source = x_ref if layer == 0 else near.at[1]
        for index in range(len(HALOS)):
            halo_copy(layer, index, source).wait_send()
        pltpu.make_async_copy(far.at[layer], far.at[layer], far_send.at[layer]).wait()


def per_device(stream_in, norm_gains, w_inner, w_outer):
    hbm = pl.BlockSpec(memory_space=pl.ANY)
    return pl.pallas_call(
        body,
        out_shape=jax.ShapeDtypeStruct(stream_in.shape, stream_in.dtype),
        in_specs=[hbm, pl.BlockSpec(memory_space=pltpu.VMEM), hbm, hbm],
        out_specs=hbm,
        scratch_shapes=[
            pltpu.VMEM((LAYERS, NEAR_ROWS, PAD + COLS), jnp.bfloat16),
            pltpu.VMEM((LAYERS, FAR_ROWS, COLS), jnp.bfloat16),
            pltpu.VMEM((FAR_ROWS, COLS), jnp.bfloat16),
            pltpu.VMEM((LAYERS, DIM, LANES), jnp.float32),
            pltpu.VMEM((LAYERS, HID, DIM), jnp.bfloat16),
            pltpu.VMEM((LAYERS, DIM, HID), jnp.bfloat16),
            pltpu.VMEM((LAYERS, DIM, HID), jnp.bfloat16),
            pltpu.VMEM((LAYERS, HID, DIM), jnp.bfloat16),
            pltpu.VMEM((DIM, SUB), jnp.float32),
            pltpu.VMEM((2, DIM, CHUNK), jnp.bfloat16),
            pltpu.SemaphoreType.DMA,
            pltpu.SemaphoreType.DMA((2,)),
            pltpu.SemaphoreType.DMA((LAYERS,)),
            pltpu.SemaphoreType.DMA((LAYERS, CHUNKS)),
            pltpu.SemaphoreType.DMA((LAYERS, len(HALOS))),
            pltpu.SemaphoreType.DMA((LAYERS, len(HALOS))),
            pltpu.SemaphoreType.DMA((2,)),
        ],
        compiler_params=pltpu.CompilerParams(
            collective_id=0, has_side_effects=True, vmem_limit_bytes=60 * 1024 * 1024
        ),
    )(stream_in, norm_gains, w_inner, w_outer)


def solution(mesh):
    return jax.shard_map(
        per_device,
        mesh=mesh,
        in_specs=(P(None, ("batch", "seq")), P(), P(), P()),
        out_specs=P(None, ("batch", "seq")),
        check_vma=False,
    )
```

```python
import functools

import jax
import jax.numpy as jnp
from jax import lax
from jax.experimental import pallas as pl
from jax.experimental.pallas import tpu as pltpu
from jax.sharding import PartitionSpec as P

TRACKS = 20
WIDTH = 16
LAYERS = 2
DIM = 320
HID = 640
RING = 128
COLS = 8192
NEAR = 13
NEAR_ROWS = NEAR * WIDTH
FAR_ROWS = DIM - NEAR_ROWS
PAD = 4096
CHUNKS = 8
CHUNK = COLS // CHUNKS
SUB = 512
LANES = 128
FAR = tuple(2**e for e in range(TRACKS - NEAR))
HOP2, HOP8, HOP16 = range(3)
HOP_TRACK = (1, 3, 4)
LEAD = 2

HALOS = (
    (0, 128, 128, 7),
    (128, 16, 256, 7),
    (144, 16, 512, 7),
    (192, 16, 1024, 4),
    (192, 16, 1024, 5),
    (176, 32, 1024, 6),
    (160, 48, 1024, 7),
)


def halo_slices(index):
    row, rows, cols, chunk = HALOS[index]
    start = (chunk + 1) * CHUNK - cols
    return pl.ds(row, rows), start, cols


def body(
    x_ref, gain_ref, inner_ref, outer_ref, out_ref,
    near, far, made, hop, gains, inner_t, inner_raw, outer_t, rotated, staged,
    local_sem, weight_sem, far_send, far_recv, hop_send, hop_recv, halo_send, halo_recv, out_sem,
):
    me = lax.axis_index("seq")
    row, depth = me // 32, lax.rem(me // 4, 8)
    half, core = lax.rem(me // 2, 2), lax.rem(me, 2)

    def device(y, z, x):
        return ((lax.rem(y + 4, 4) * 8 + lax.rem(z + 8, 8)) * 2 + x) * 2 + core

    ahead = [lax.rem(me + d, RING) for d in FAR]
    behind = [lax.rem(me + RING - d, RING) for d in FAR]
    deep = jnp.where(depth >= 4, 1, 0)
    last = jnp.where(depth == 7, 1, 0)
    hop_to = [
        device(row + last * half, depth, 1 - half),
        device(row + 1, depth, half),
        device(row + deep, depth - 2, half),
    ]
    hop_from = [
        device(row - last * (1 - half), depth, 1 - half),
        device(row - 1, depth, half),
        device(row - jnp.where(lax.rem(depth + 2, 8) >= 4, 1, 0), depth + 2, half),
    ]
    pass_to = [device(row, depth + 1, half), device(row, depth + 2, half), device(row, depth - 2, half)]
    pass_from = [device(row, depth - 1, half), device(row, depth - 2, half), device(row, depth + 2, half)]
    sends_hop = [half == 1, depth == 6, None]
    passes = [half == 0, depth == 6, None]

    def where(condition, action):
        if condition is None:
            action()
        else:
            pl.when(condition)(action)

    near_copy = pltpu.make_async_copy(
        x_ref.at[pl.ds(0, NEAR_ROWS), :], near.at[0, :, pl.ds(PAD, COLS)], local_sem
    )
    near_copy.start()
    inner_copy = pltpu.make_async_copy(inner_ref, inner_raw, weight_sem.at[0])
    outer_copy = pltpu.make_async_copy(outer_ref, outer_t, weight_sem.at[1])
    inner_copy.start()
    outer_copy.start()

    barrier = pltpu.get_barrier_semaphore()
    peers = ahead + behind + hop_to + hop_from + pass_to + pass_from
    for peer in peers:
        pl.semaphore_signal(barrier, inc=1, device_id={"seq": peer})
    pl.semaphore_wait(barrier, len(peers))

    def halo_copy(layer, index, source):
        rows, start, cols = halo_slices(index)
        return pltpu.make_async_remote_copy(
            src_ref=source.at[rows, pl.ds(start + (0 if layer == 0 else PAD), cols)],
            dst_ref=near.at[layer, rows, pl.ds(start + PAD - COLS, cols)],
            send_sem=halo_send.at[layer, index],
            recv_sem=halo_recv.at[layer, index],
            device_id={"seq": ahead[0]},
        )

    def far_copy(layer, track, chunk, source, base):
        cols = pl.ds(pl.multiple_of(chunk * CHUNK, CHUNK), CHUNK)
        return pltpu.make_async_remote_copy(
            src_ref=source.at[pl.ds(base + track * WIDTH, WIDTH), cols],
            dst_ref=far.at[layer, pl.ds(track * WIDTH, WIDTH), cols],
            send_sem=far_send.at[layer],
            recv_sem=far_recv.at[layer, chunk],
            device_id={"seq": ahead[track]},
        )

    def hop_copy(layer, kind, chunk, source, base):
        cols = pl.ds(pl.multiple_of(chunk * CHUNK, CHUNK), CHUNK)
        return pltpu.make_async_remote_copy(
            src_ref=source.at[pl.ds(base + HOP_TRACK[kind] * WIDTH, WIDTH), cols],
            dst_ref=hop.at[layer, kind, :, cols],
            send_sem=far_send.at[layer],
            recv_sem=hop_recv.at[layer, kind, chunk],
            device_id={"seq": hop_to[kind]},
        )

    def pass_copy(layer, kind, chunk):
        cols = pl.ds(pl.multiple_of(chunk * CHUNK, CHUNK), CHUNK)
        return pltpu.make_async_remote_copy(
            src_ref=hop.at[layer, kind, :, cols],
            dst_ref=far.at[layer, pl.ds(HOP_TRACK[kind] * WIDTH, WIDTH), cols],
            send_sem=hop_send.at[layer, kind],
            recv_sem=far_recv.at[layer, chunk],
            device_id={"seq": pass_to[kind]},
        )

    def send_far(layer, chunk, source, base):
        for kind in (HOP16, HOP8, HOP2):
            where(sends_hop[kind], lambda: hop_copy(layer, kind, chunk, source, base).start())
        for track in range(len(FAR)):
            kind = HOP_TRACK.index(track) if track in HOP_TRACK else None
            if kind == HOP16:
                continue
            direct = None if kind is None else jnp.logical_not(sends_hop[kind])
            where(direct, lambda: far_copy(layer, track, chunk, source, base).start())

    def forward(layer, chunk):
        cols = pl.ds(pl.multiple_of(chunk * CHUNK, CHUNK), CHUNK)
        for kind in (HOP16, HOP8, HOP2):
            def relay():
                landed = hop.at[layer, kind, :, cols]
                pltpu.make_async_copy(landed, landed, hop_recv.at[layer, kind, chunk]).wait()
                pass_copy(layer, kind, chunk).start()

            where(passes[kind], relay)

    for index in range(len(HALOS)):
        halo_copy(0, index, x_ref).start()

    @pl.loop(0, CHUNKS)
    def _(step):
        send_far(0, lax.rem(step + CHUNKS // 2, CHUNKS), x_ref, NEAR_ROWS)

    for layer in range(LAYERS):
        gains[layer] = jnp.broadcast_to(gain_ref[layer : layer + 1, :], (LANES, DIM)).T
    inner_copy.wait()
    for layer in range(LAYERS):
        inner_t[layer] = inner_raw[layer].T
    outer_copy.wait()
    near_copy.wait()

    def mix(layer, at, store):
        base = pl.multiple_of(PAD + at, LANES)
        for track in range(NEAR):
            shift = 2**track
            rows = pl.ds(track * WIDTH, WIDTH)
            if shift < LANES:
                wide = near[layer, rows, pl.ds(pl.multiple_of(base - LANES, LANES), SUB + LANES)]
                piece = pltpu.roll(wide.astype(jnp.float32), shift, 1)[:, LANES:]
            else:
                piece = near[layer, rows, pl.ds(pl.multiple_of(base - shift, LANES), SUB)].astype(jnp.float32)
            rotated[rows, :] = piece
        rotated[NEAR_ROWS:, :] = far[layer, :, pl.ds(pl.multiple_of(at, LANES), SUB)].astype(jnp.float32)
        values = rotated[...]
        average = jnp.sum(values, axis=0, keepdims=True) * (1.0 / DIM)
        centred = values - average
        spread = jnp.sum(centred * centred, axis=0, keepdims=True) * (1.0 / DIM)
        scale = lax.rsqrt(spread + 1e-05)
        gain = jnp.concatenate([gains[layer]] * (SUB // LANES), axis=1)
        normed = (centred * scale * gain).astype(jnp.bfloat16)
        inner_sum = jnp.dot(inner_t[layer], normed, preferred_element_type=jnp.float32)
        hidden = (0.5 * inner_sum * (1.0 + lax.erf(inner_sum * (0.5**0.5)))).astype(jnp.bfloat16)
        outer_sum = jnp.dot(outer_t[layer], hidden, preferred_element_type=jnp.float32)
        store((rotated[...] + outer_sum).astype(jnp.bfloat16))

    def wait_far(layer, chunk):
        cols = pl.ds(pl.multiple_of(chunk * CHUNK, CHUNK), CHUNK)
        whole = far.at[layer, :, cols]
        pltpu.make_async_copy(whole, whole, far_recv.at[layer, chunk]).wait()

    def wait_halos(layer, source):
        for index in range(len(HALOS)):
            halo_copy(layer, index, source).wait_recv()

    def turn(step):
        return lax.rem(step + CHUNKS // 2, CHUNKS)

    for step in range(LEAD):
        forward(0, turn(step))

    @pl.loop(0, CHUNKS)
    def _(step):
        chunk = turn(step)

        @pl.when(step < CHUNKS - LEAD)
        def _():
            forward(0, turn(step + LEAD))

        @pl.when(step >= CHUNKS // 2)
        def _():
            forward(1, turn(step - CHUNKS // 2))

        wait_far(0, chunk)

        @pl.when(step == CHUNKS // 2)
        def _():
            wait_halos(0, x_ref)

        @pl.loop(0, CHUNK // SUB)
        def _(part):
            at = pl.multiple_of(chunk * CHUNK + part * SUB, SUB)

            def store(result):
                near[1, :, pl.ds(pl.multiple_of(PAD + at, SUB), SUB)] = result[:NEAR_ROWS]
                made[:, pl.ds(at, SUB)] = result[NEAR_ROWS:]

            mix(0, at, store)

        send_far(1, chunk, made, 0)
        for index, halo in enumerate(HALOS):
            @pl.when(chunk == halo[3])
            def _():
                halo_copy(1, index, near.at[1]).start()

    def out_copy(slot, chunk):
        cols = pl.ds(pl.multiple_of(chunk * CHUNK, CHUNK), CHUNK)
        return pltpu.make_async_copy(staged.at[slot], out_ref.at[:, cols], out_sem.at[slot])

    @pl.loop(0, CHUNKS)
    def _(step):
        chunk = lax.rem(step + CHUNKS // 2, CHUNKS)
        slot = lax.rem(step, 2)

        @pl.when(step < CHUNKS // 2)
        def _():
            forward(1, turn(step + CHUNKS // 2))

        wait_far(1, chunk)

        @pl.when(step == CHUNKS // 2)
        def _():
            wait_halos(1, near.at[1])

        @pl.when(step >= 2)
        def _():
            out_copy(slot, chunk).wait()

        @pl.loop(0, CHUNK // SUB)
        def _(part):
            at = pl.multiple_of(chunk * CHUNK + part * SUB, SUB)

            def store(result):
                staged[slot, :, pl.ds(pl.multiple_of(part * SUB, SUB), SUB)] = result

            mix(1, at, store)

        out_copy(slot, chunk).start()

    out_copy(0, 0).wait()
    out_copy(1, 0).wait()
    for layer in range(LAYERS):
        source = x_ref if layer == 0 else near.at[1]
        for index in range(len(HALOS)):
            halo_copy(layer, index, source).wait_send()
        pltpu.make_async_copy(far.at[layer], far.at[layer], far_send.at[layer]).wait()
        for kind in (HOP16, HOP8, HOP2):
            kept = hop.at[layer, kind]
            where(passes[kind], lambda: pltpu.make_async_copy(kept, kept, hop_send.at[layer, kind]).wait())


def per_device(stream_in, norm_gains, w_inner, w_outer):
    hbm = pl.BlockSpec(memory_space=pl.ANY)
    return pl.pallas_call(
        body,
        out_shape=jax.ShapeDtypeStruct(stream_in.shape, stream_in.dtype),
        in_specs=[hbm, pl.BlockSpec(memory_space=pltpu.VMEM), hbm, hbm],
        out_specs=hbm,
        scratch_shapes=[
            pltpu.VMEM((LAYERS, NEAR_ROWS, PAD + COLS), jnp.bfloat16),
            pltpu.VMEM((LAYERS, FAR_ROWS, COLS), jnp.bfloat16),
            pltpu.VMEM((FAR_ROWS, COLS), jnp.bfloat16),
            pltpu.VMEM((LAYERS, 3, WIDTH, COLS), jnp.bfloat16),
            pltpu.VMEM((LAYERS, DIM, LANES), jnp.float32),
            pltpu.VMEM((LAYERS, HID, DIM), jnp.bfloat16),
            pltpu.VMEM((LAYERS, DIM, HID), jnp.bfloat16),
            pltpu.VMEM((LAYERS, DIM, HID), jnp.bfloat16),
            pltpu.VMEM((DIM, SUB), jnp.float32),
            pltpu.VMEM((2, DIM, CHUNK), jnp.bfloat16),
            pltpu.SemaphoreType.DMA,
            pltpu.SemaphoreType.DMA((2,)),
            pltpu.SemaphoreType.DMA((LAYERS,)),
            pltpu.SemaphoreType.DMA((LAYERS, CHUNKS)),
            pltpu.SemaphoreType.DMA((LAYERS, 3)),
            pltpu.SemaphoreType.DMA((LAYERS, 3, CHUNKS)),
            pltpu.SemaphoreType.DMA((LAYERS, len(HALOS))),
            pltpu.SemaphoreType.DMA((LAYERS, len(HALOS))),
            pltpu.SemaphoreType.DMA((2,)),
        ],
        compiler_params=pltpu.CompilerParams(
            collective_id=0, has_side_effects=True, vmem_limit_bytes=60 * 1024 * 1024
        ),
    )(stream_in, norm_gains, w_inner, jnp.swapaxes(w_outer, 1, 2))


def solution(mesh):
    return jax.shard_map(
        per_device,
        mesh=mesh,
        in_specs=(P(None, ("batch", "seq")), P(), P(), P()),
        out_specs=P(None, ("batch", "seq")),
        check_vma=False,
    )
```

```python
import functools

import jax
import jax.numpy as jnp
from jax import lax
from jax.experimental import pallas as pl
from jax.experimental.pallas import tpu as pltpu
from jax.sharding import PartitionSpec as P

TRACKS = 20
WIDTH = 16
LAYERS = 2
DIM = 320
HID = 640
RING = 128
COLS = 8192
NEAR = 13
NEAR_ROWS = NEAR * WIDTH
FAR_ROWS = DIM - NEAR_ROWS
PAD = 4096
CHUNKS = 8
CHUNK = COLS // CHUNKS
SUB = 512
LANES = 128
FAR = tuple(2**e for e in range(TRACKS - NEAR))
HOP2, HOP8, HOP16 = range(3)
HOP_TRACK = (1, 3, 4)
WINDOW = 5
LEAD = 3
LAG = 4


def tails():
    pieces = [(0, 8 * WIDTH, LANES, CHUNKS - 1)]
    for track in range(8, NEAR):
        if 2**track < CHUNK:
            pieces.append((track * WIDTH, WIDTH, 2**track, CHUNKS - 1))
    for chunk in range(CHUNKS):
        need = [track for track in range(NEAR) if CHUNK <= 2**track and COLS - 2**track <= chunk * CHUNK]
        if need:
            pieces.append((need[0] * WIDTH, NEAR_ROWS - need[0] * WIDTH, CHUNK, chunk))
    return tuple(pieces)


HALOS = tails()


def halo_slices(index):
    row, rows, cols, chunk = HALOS[index]
    start = (chunk + 1) * CHUNK - cols
    return pl.ds(row, rows), start, cols


def body(
    x_ref, gain_ref, inner_ref, outer_ref, out_ref,
    near, far, made, hop, gains, inner_t, inner_raw, outer_t, rotated,
    local_sem, weight_sem, far_send, far_recv, hop_send, hop_recv, halo_send, halo_recv,
):
    me = lax.axis_index("seq")
    row, depth = me // 32, lax.rem(me // 4, 8)
    half, core = lax.rem(me // 2, 2), lax.rem(me, 2)

    def device(y, z, x):
        return ((lax.rem(y + 4, 4) * 8 + lax.rem(z + 8, 8)) * 2 + x) * 2 + core

    ahead = [lax.rem(me + d, RING) for d in FAR]
    behind = [lax.rem(me + RING - d, RING) for d in FAR]
    deep = jnp.where(depth >= 4, 1, 0)
    last = jnp.where(depth == 7, 1, 0)
    hop_to = [
        device(row + last * half, depth, 1 - half),
        device(row + 1, depth, half),
        device(row + deep, depth - 2, half),
    ]
    hop_from = [
        device(row - last * (1 - half), depth, 1 - half),
        device(row - 1, depth, half),
        device(row - jnp.where(lax.rem(depth + 2, 8) >= 4, 1, 0), depth + 2, half),
    ]
    pass_to = [device(row, depth + 1, half), device(row, depth + 2, half), device(row, depth - 2, half)]
    pass_from = [device(row, depth - 1, half), device(row, depth - 2, half), device(row, depth + 2, half)]
    sends_hop = [half == 1, depth == 6, None]
    passes = [half == 0, depth == 6, None]

    def where(condition, action):
        if condition is None:
            action()
        else:
            pl.when(condition)(action)

    near_copy = pltpu.make_async_copy(
        x_ref.at[pl.ds(0, NEAR_ROWS), :], near.at[0, :, pl.ds(PAD, COLS)], local_sem
    )
    near_copy.start()
    inner_copy = pltpu.make_async_copy(inner_ref, inner_raw, weight_sem.at[0])
    outer_copy = pltpu.make_async_copy(outer_ref, outer_t, weight_sem.at[1])
    inner_copy.start()
    outer_copy.start()

    barrier = pltpu.get_barrier_semaphore()
    peers = ahead + behind + hop_to + hop_from + pass_to + pass_from
    for peer in peers:
        pl.semaphore_signal(barrier, inc=1, device_id={"seq": peer})
    pl.semaphore_wait(barrier, len(peers))

    def halo_copy(layer, index, source):
        rows, start, cols = halo_slices(index)
        return pltpu.make_async_remote_copy(
            src_ref=source.at[rows, pl.ds(start + (0 if layer == 0 else PAD), cols)],
            dst_ref=near.at[layer, rows, pl.ds(start + PAD - COLS, cols)],
            send_sem=halo_send.at[layer, index],
            recv_sem=halo_recv.at[layer, index],
            device_id={"seq": ahead[0]},
        )

    def far_copy(layer, track, chunk, source, base):
        cols = pl.ds(pl.multiple_of(chunk * CHUNK, CHUNK), CHUNK)
        return pltpu.make_async_remote_copy(
            src_ref=source.at[pl.ds(base + track * WIDTH, WIDTH), cols],
            dst_ref=far.at[layer, pl.ds(track * WIDTH, WIDTH), cols],
            send_sem=far_send.at[layer],
            recv_sem=far_recv.at[layer, chunk],
            device_id={"seq": ahead[track]},
        )

    def hop_copy(layer, kind, chunk, source, base):
        cols = pl.ds(pl.multiple_of(chunk * CHUNK, CHUNK), CHUNK)
        return pltpu.make_async_remote_copy(
            src_ref=source.at[pl.ds(base + HOP_TRACK[kind] * WIDTH, WIDTH), cols],
            dst_ref=hop.at[layer, kind, :, cols],
            send_sem=far_send.at[layer],
            recv_sem=hop_recv.at[layer, kind, chunk],
            device_id={"seq": hop_to[kind]},
        )

    def pass_copy(layer, kind, chunk):
        cols = pl.ds(pl.multiple_of(chunk * CHUNK, CHUNK), CHUNK)
        return pltpu.make_async_remote_copy(
            src_ref=hop.at[layer, kind, :, cols],
            dst_ref=far.at[layer, pl.ds(HOP_TRACK[kind] * WIDTH, WIDTH), cols],
            send_sem=hop_send.at[layer, kind],
            recv_sem=far_recv.at[layer, chunk],
            device_id={"seq": pass_to[kind]},
        )

    def send_far(layer, chunk, source, base):
        for kind in (HOP16, HOP8, HOP2):
            where(sends_hop[kind], lambda: hop_copy(layer, kind, chunk, source, base).start())
        for track in range(len(FAR)):
            kind = HOP_TRACK.index(track) if track in HOP_TRACK else None
            if kind == HOP16:
                continue
            direct = None if kind is None else jnp.logical_not(sends_hop[kind])
            where(direct, lambda: far_copy(layer, track, chunk, source, base).start())

    def forward(layer, chunk):
        cols = pl.ds(pl.multiple_of(chunk * CHUNK, CHUNK), CHUNK)
        for kind in (HOP16, HOP8, HOP2):
            def relay():
                landed = hop.at[layer, kind, :, cols]
                pltpu.make_async_copy(landed, landed, hop_recv.at[layer, kind, chunk]).wait()
                pass_copy(layer, kind, chunk).start()

            where(passes[kind], relay)

    for index in range(len(HALOS)):
        halo_copy(0, index, x_ref).start()

    def turn(step):
        return lax.rem(step + CHUNKS // 2, CHUNKS)

    @pl.loop(0, WINDOW)
    def _(step):
        send_far(0, turn(step), x_ref, NEAR_ROWS)

    for layer in range(LAYERS):
        gains[layer] = jnp.broadcast_to(gain_ref[layer : layer + 1, :], (LANES, DIM)).T
    inner_copy.wait()
    for layer in range(LAYERS):
        inner_t[layer] = inner_raw[layer].T
    outer_copy.wait()
    near_copy.wait()

    def mix(layer, at, store):
        base = pl.multiple_of(PAD + at, LANES)
        for track in range(NEAR):
            shift = 2**track
            rows = pl.ds(track * WIDTH, WIDTH)
            if shift < LANES:
                wide = near[layer, rows, pl.ds(pl.multiple_of(base - LANES, LANES), SUB + LANES)]
                piece = pltpu.roll(wide.astype(jnp.float32), shift, 1)[:, LANES:]
            else:
                piece = near[layer, rows, pl.ds(pl.multiple_of(base - shift, LANES), SUB)].astype(jnp.float32)
            rotated[rows, :] = piece
        rotated[NEAR_ROWS:, :] = far[layer, :, pl.ds(pl.multiple_of(at, LANES), SUB)].astype(jnp.float32)
        values = rotated[...]
        average = jnp.sum(values, axis=0, keepdims=True) * (1.0 / DIM)
        centred = values - average
        spread = jnp.sum(centred * centred, axis=0, keepdims=True) * (1.0 / DIM)
        scale = lax.rsqrt(spread + 1e-05)
        gain = jnp.concatenate([gains[layer]] * (SUB // LANES), axis=1)
        normed = (centred * scale * gain).astype(jnp.bfloat16)
        inner_sum = jnp.dot(inner_t[layer], normed, preferred_element_type=jnp.float32)
        hidden = (0.5 * inner_sum * (1.0 + lax.erf(inner_sum * (0.5**0.5)))).astype(jnp.bfloat16)
        outer_sum = jnp.dot(outer_t[layer], hidden, preferred_element_type=jnp.float32)
        store((rotated[...] + outer_sum).astype(jnp.bfloat16))

    def wait_far(layer, chunk):
        cols = pl.ds(pl.multiple_of(chunk * CHUNK, CHUNK), CHUNK)
        whole = far.at[layer, :, cols]
        pltpu.make_async_copy(whole, whole, far_recv.at[layer, chunk]).wait()

    def wait_halos(layer, source):
        for index in range(len(HALOS)):
            halo_copy(layer, index, source).wait_recv()

    for step in range(LEAD):
        forward(0, turn(step))

    @pl.loop(0, CHUNKS)
    def _(step):
        chunk = turn(step)

        @pl.when(step < CHUNKS - WINDOW)
        def _():
            send_far(0, turn(step + WINDOW), x_ref, NEAR_ROWS)

        @pl.when(step < CHUNKS - LEAD)
        def _():
            forward(0, turn(step + LEAD))

        @pl.when(step >= LAG)
        def _():
            forward(1, turn(step - LAG))

        wait_far(0, chunk)

        @pl.when(step == CHUNKS // 2)
        def _():
            wait_halos(0, x_ref)

        @pl.loop(0, CHUNK // SUB)
        def _(part):
            at = pl.multiple_of(chunk * CHUNK + part * SUB, SUB)

            def store(result):
                near[1, :, pl.ds(pl.multiple_of(PAD + at, SUB), SUB)] = result[:NEAR_ROWS]
                made[:, pl.ds(at, SUB)] = result[NEAR_ROWS:]

            mix(0, at, store)

        send_far(1, chunk, made, 0)
        for index, halo in enumerate(HALOS):
            @pl.when(chunk == halo[3])
            def _():
                halo_copy(1, index, near.at[1]).start()

    @pl.loop(0, CHUNKS)
    def _(step):
        chunk = lax.rem(step + CHUNKS // 2, CHUNKS)

        @pl.when(step < LAG)
        def _():
            forward(1, turn(step + CHUNKS - LAG))

        wait_far(1, chunk)

        @pl.when(step == CHUNKS // 2)
        def _():
            wait_halos(1, near.at[1])

        @pl.loop(0, CHUNK // SUB)
        def _(part):
            at = pl.multiple_of(chunk * CHUNK + part * SUB, SUB)

            def store(result):
                out_ref[:, pl.ds(at, SUB)] = result

            mix(1, at, store)

    for layer in range(LAYERS):
        source = x_ref if layer == 0 else near.at[1]
        for index in range(len(HALOS)):
            halo_copy(layer, index, source).wait_send()
        pltpu.make_async_copy(far.at[layer], far.at[layer], far_send.at[layer]).wait()
        for kind in (HOP16, HOP8, HOP2):
            kept = hop.at[layer, kind]
            where(passes[kind], lambda: pltpu.make_async_copy(kept, kept, hop_send.at[layer, kind]).wait())


def per_device(stream_in, norm_gains, w_inner, w_outer):
    hbm = pl.BlockSpec(memory_space=pltpu.HBM)
    vmem = pl.BlockSpec(memory_space=pltpu.VMEM)
    return pl.pallas_call(
        body,
        out_shape=pltpu.VMEM(stream_in.shape, stream_in.dtype),
        in_specs=[hbm, vmem, hbm, hbm],
        out_specs=vmem,
        scratch_shapes=[
            pltpu.VMEM((LAYERS, NEAR_ROWS, PAD + COLS), jnp.bfloat16),
            pltpu.VMEM((LAYERS, FAR_ROWS, COLS), jnp.bfloat16),
            pltpu.VMEM((FAR_ROWS, COLS), jnp.bfloat16),
            pltpu.VMEM((LAYERS, 3, WIDTH, COLS), jnp.bfloat16),
            pltpu.VMEM((LAYERS, DIM, LANES), jnp.float32),
            pltpu.VMEM((LAYERS, HID, DIM), jnp.bfloat16),
            pltpu.VMEM((LAYERS, DIM, HID), jnp.bfloat16),
            pltpu.VMEM((LAYERS, DIM, HID), jnp.bfloat16),
            pltpu.VMEM((DIM, SUB), jnp.float32),
            pltpu.SemaphoreType.DMA,
            pltpu.SemaphoreType.DMA((2,)),
            pltpu.SemaphoreType.DMA((LAYERS,)),
            pltpu.SemaphoreType.DMA((LAYERS, CHUNKS)),
            pltpu.SemaphoreType.DMA((LAYERS, 3)),
            pltpu.SemaphoreType.DMA((LAYERS, 3, CHUNKS)),
            pltpu.SemaphoreType.DMA((LAYERS, len(HALOS))),
            pltpu.SemaphoreType.DMA((LAYERS, len(HALOS))),
        ],
        compiler_params=pltpu.CompilerParams(
            collective_id=0, has_side_effects=True, vmem_limit_bytes=61_600_000
        ),
    )(stream_in, norm_gains, w_inner, jnp.swapaxes(w_outer, 1, 2))


def solution(mesh):
    return jax.shard_map(
        per_device,
        mesh=mesh,
        in_specs=(P(None, ("batch", "seq")), P(), P(), P()),
        out_specs=P(None, ("batch", "seq")),
        check_vma=False,
    )
```

```python
import functools

import jax
import jax.numpy as jnp
from jax import lax
from jax.experimental import pallas as pl
from jax.experimental.pallas import tpu as pltpu
from jax.sharding import PartitionSpec as P

TRACKS = 20
WIDTH = 16
LAYERS = 2
DIM = 320
HID = 640
RING = 128
COLS = 8192
NEAR = 13
NEAR_ROWS = NEAR * WIDTH
FAR_ROWS = DIM - NEAR_ROWS
PAD = 4096
CHUNKS = 8
CHUNK = COLS // CHUNKS
SUB = 1024
LANES = 128
LAST = CHUNKS // 2 - 1
VMEM_BODY = 57_000_000
FAR = tuple(2**e for e in range(TRACKS - NEAR))
HOP2, HOP8, HOP16 = range(3)
HOP_TRACK = (1, 3, 4)
WINDOW = 5
LEAD = 3
LAG = 4


def tails():
    pieces = [(0, 8 * WIDTH, LANES, CHUNKS - 1)]
    for track in range(8, NEAR):
        if 2**track < CHUNK:
            pieces.append((track * WIDTH, WIDTH, 2**track, CHUNKS - 1))
    for chunk in range(CHUNKS):
        need = [track for track in range(NEAR) if CHUNK <= 2**track and COLS - 2**track <= chunk * CHUNK]
        if need:
            pieces.append((need[0] * WIDTH, NEAR_ROWS - need[0] * WIDTH, CHUNK, chunk))
    return tuple(pieces)


HALOS = tails()


def halo_slices(index):
    row, rows, cols, chunk = HALOS[index]
    start = (chunk + 1) * CHUNK - cols
    return pl.ds(row, rows), start, cols


def blend(rotated, gain, inner_t, outer_t):
    values = rotated[...]
    average = jnp.sum(values, axis=0, keepdims=True) * (1.0 / DIM)
    centred = values - average
    spread = jnp.sum(centred * centred, axis=0, keepdims=True) * (1.0 / DIM)
    scale = lax.rsqrt(spread + 1e-05)
    gain = jnp.concatenate([gain] * (SUB // LANES), axis=1)
    normed = (centred * scale * gain).astype(jnp.bfloat16)
    inner_sum = jnp.dot(inner_t, normed, preferred_element_type=jnp.float32)
    hidden = (0.5 * inner_sum * (1.0 + lax.erf(inner_sum * (0.5**0.5)))).astype(jnp.bfloat16)
    outer_sum = jnp.dot(outer_t, hidden, preferred_element_type=jnp.float32)
    return (rotated[...] + outer_sum).astype(jnp.bfloat16)


def body(
    x_ref, gain_ref, inner_ref, outer_ref, out_ref, rest_ref, gains, inner_t, outer_t,
    near, far, made, hop, inner_raw, rotated,
    local_sem, weight_sem, far_send, far_recv, hop_send, hop_recv, halo_send, halo_recv,
):
    me = lax.axis_index("seq")
    row, depth = me // 32, lax.rem(me // 4, 8)
    half, core = lax.rem(me // 2, 2), lax.rem(me, 2)

    def device(y, z, x):
        return ((lax.rem(y + 4, 4) * 8 + lax.rem(z + 8, 8)) * 2 + x) * 2 + core

    ahead = [lax.rem(me + d, RING) for d in FAR]
    behind = [lax.rem(me + RING - d, RING) for d in FAR]
    deep = jnp.where(depth >= 4, 1, 0)
    last = jnp.where(depth == 7, 1, 0)
    hop_to = [
        device(row + last * half, depth, 1 - half),
        device(row + 1, depth, half),
        device(row + deep, depth - 2, half),
    ]
    hop_from = [
        device(row - last * (1 - half), depth, 1 - half),
        device(row - 1, depth, half),
        device(row - jnp.where(lax.rem(depth + 2, 8) >= 4, 1, 0), depth + 2, half),
    ]
    pass_to = [device(row, depth + 1, half), device(row, depth + 2, half), device(row, depth - 2, half)]
    pass_from = [device(row, depth - 1, half), device(row, depth - 2, half), device(row, depth + 2, half)]
    sends_hop = [half == 1, depth == 6, None]
    passes = [half == 0, depth == 6, None]

    def where(condition, action):
        if condition is None:
            action()
        else:
            pl.when(condition)(action)

    near_copy = pltpu.make_async_copy(
        x_ref.at[pl.ds(0, NEAR_ROWS), :], near.at[0, :, pl.ds(PAD, COLS)], local_sem
    )
    near_copy.start()
    inner_copy = pltpu.make_async_copy(inner_ref, inner_raw, weight_sem.at[0])
    outer_copy = pltpu.make_async_copy(outer_ref, outer_t, weight_sem.at[1])
    inner_copy.start()
    outer_copy.start()

    barrier = pltpu.get_barrier_semaphore()
    peers = ahead + behind + hop_to + hop_from + pass_to + pass_from
    for peer in peers:
        pl.semaphore_signal(barrier, inc=1, device_id={"seq": peer})
    pl.semaphore_wait(barrier, len(peers))

    def halo_copy(layer, index, source):
        rows, start, cols = halo_slices(index)
        return pltpu.make_async_remote_copy(
            src_ref=source.at[rows, pl.ds(start + (0 if layer == 0 else PAD), cols)],
            dst_ref=near.at[layer, rows, pl.ds(start + PAD - COLS, cols)],
            send_sem=halo_send.at[layer, index],
            recv_sem=halo_recv.at[layer, index],
            device_id={"seq": ahead[0]},
        )

    def far_copy(layer, track, chunk, source, base):
        cols = pl.ds(pl.multiple_of(chunk * CHUNK, CHUNK), CHUNK)
        return pltpu.make_async_remote_copy(
            src_ref=source.at[pl.ds(base + track * WIDTH, WIDTH), cols],
            dst_ref=far.at[layer, pl.ds(track * WIDTH, WIDTH), cols],
            send_sem=far_send.at[layer],
            recv_sem=far_recv.at[layer, chunk],
            device_id={"seq": ahead[track]},
        )

    def hop_copy(layer, kind, chunk, source, base):
        cols = pl.ds(pl.multiple_of(chunk * CHUNK, CHUNK), CHUNK)
        return pltpu.make_async_remote_copy(
            src_ref=source.at[pl.ds(base + HOP_TRACK[kind] * WIDTH, WIDTH), cols],
            dst_ref=hop.at[layer, kind, :, cols],
            send_sem=far_send.at[layer],
            recv_sem=hop_recv.at[layer, kind, chunk],
            device_id={"seq": hop_to[kind]},
        )

    def pass_copy(layer, kind, chunk):
        cols = pl.ds(pl.multiple_of(chunk * CHUNK, CHUNK), CHUNK)
        return pltpu.make_async_remote_copy(
            src_ref=hop.at[layer, kind, :, cols],
            dst_ref=far.at[layer, pl.ds(HOP_TRACK[kind] * WIDTH, WIDTH), cols],
            send_sem=hop_send.at[layer, kind],
            recv_sem=far_recv.at[layer, chunk],
            device_id={"seq": pass_to[kind]},
        )

    def send_far(layer, chunk, source, base):
        for kind in (HOP16, HOP8, HOP2):
            where(sends_hop[kind], lambda: hop_copy(layer, kind, chunk, source, base).start())
        for track in range(len(FAR)):
            kind = HOP_TRACK.index(track) if track in HOP_TRACK else None
            if kind == HOP16:
                continue
            direct = None if kind is None else jnp.logical_not(sends_hop[kind])
            where(direct, lambda: far_copy(layer, track, chunk, source, base).start())

    def forward(layer, chunk):
        cols = pl.ds(pl.multiple_of(chunk * CHUNK, CHUNK), CHUNK)
        for kind in (HOP16, HOP8, HOP2):
            def relay():
                landed = hop.at[layer, kind, :, cols]
                pltpu.make_async_copy(landed, landed, hop_recv.at[layer, kind, chunk]).wait()
                pass_copy(layer, kind, chunk).start()

            where(passes[kind], relay)

    for index in range(len(HALOS)):
        halo_copy(0, index, x_ref).start()

    def turn(step):
        return lax.rem(step + CHUNKS // 2, CHUNKS)

    @pl.loop(0, WINDOW)
    def _(step):
        send_far(0, turn(step), x_ref, NEAR_ROWS)

    for layer in range(LAYERS):
        gains[layer] = jnp.broadcast_to(gain_ref[layer : layer + 1, :], (LANES, DIM)).T
    inner_copy.wait()
    for layer in range(LAYERS):
        inner_t[layer] = inner_raw[layer].T
    outer_copy.wait()
    near_copy.wait()

    def gather_near(layer, at, keep):
        base = pl.multiple_of(PAD + at, LANES)
        for track in range(NEAR):
            shift = 2**track
            rows = pl.ds(track * WIDTH, WIDTH)
            if shift < LANES:
                wide = near[layer, rows, pl.ds(pl.multiple_of(base - LANES, LANES), SUB + LANES)]
                piece = pltpu.roll(wide.astype(jnp.float32), shift, 1)[:, LANES:]
            else:
                piece = near[layer, rows, pl.ds(pl.multiple_of(base - shift, LANES), SUB)].astype(jnp.float32)
            keep(rows, piece)

    def mix(layer, at, store):
        def keep(rows, piece):
            rotated[rows, :] = piece

        gather_near(layer, at, keep)
        rotated[NEAR_ROWS:, :] = far[layer, :, pl.ds(pl.multiple_of(at, LANES), SUB)].astype(jnp.float32)
        store(blend(rotated, gains[layer], inner_t[layer], outer_t[layer]))

    def wait_far(layer, chunk):
        cols = pl.ds(pl.multiple_of(chunk * CHUNK, CHUNK), CHUNK)
        whole = far.at[layer, :, cols]
        pltpu.make_async_copy(whole, whole, far_recv.at[layer, chunk]).wait()

    def wait_halos(layer, source):
        for index in range(len(HALOS)):
            halo_copy(layer, index, source).wait_recv()

    for step in range(LEAD):
        forward(0, turn(step))

    @pl.loop(0, CHUNKS)
    def _(step):
        chunk = turn(step)

        @pl.when(step < CHUNKS - WINDOW)
        def _():
            send_far(0, turn(step + WINDOW), x_ref, NEAR_ROWS)

        @pl.when(step < CHUNKS - LEAD)
        def _():
            forward(0, turn(step + LEAD))

        @pl.when(step >= LAG)
        def _():
            forward(1, turn(step - LAG))

        wait_far(0, chunk)

        @pl.when(step == CHUNKS // 2)
        def _():
            wait_halos(0, x_ref)

        @pl.loop(0, CHUNK // SUB)
        def _(part):
            at = pl.multiple_of(chunk * CHUNK + part * SUB, SUB)

            def store(result):
                near[1, :, pl.ds(pl.multiple_of(PAD + at, SUB), SUB)] = result[:NEAR_ROWS]
                made[:, pl.ds(at, SUB)] = result[NEAR_ROWS:]

            mix(0, at, store)

        send_far(1, chunk, made, 0)
        for index, halo in enumerate(HALOS):
            @pl.when(chunk == halo[3])
            def _():
                halo_copy(1, index, near.at[1]).start()

    @pl.loop(0, CHUNKS - 1)
    def _(step):
        chunk = lax.rem(step + CHUNKS // 2, CHUNKS)

        @pl.when(step < LAG)
        def _():
            forward(1, turn(step + CHUNKS - LAG))

        wait_far(1, chunk)

        @pl.when(step == CHUNKS // 2)
        def _():
            wait_halos(1, near.at[1])

        @pl.loop(0, CHUNK // SUB)
        def _(part):
            at = pl.multiple_of(chunk * CHUNK + part * SUB, SUB)

            def store(result):
                out_ref[:, pl.ds(at, SUB)] = result

            mix(1, at, store)

    for part in range(CHUNK // SUB):
        cols = pl.ds(part * SUB, SUB)

        def keep(rows, piece):
            rest_ref[rows, cols] = piece.astype(jnp.bfloat16)

        gather_near(1, LAST * CHUNK + part * SUB, keep)

    wait_far(1, LAST)
    rest_ref[NEAR_ROWS:, :] = far[1, :, pl.ds(LAST * CHUNK, CHUNK)]
    for layer in range(LAYERS):
        source = x_ref if layer == 0 else near.at[1]
        for index in range(len(HALOS)):
            halo_copy(layer, index, source).wait_send()
        pltpu.make_async_copy(far.at[layer], far.at[layer], far_send.at[layer]).wait()
        for kind in (HOP16, HOP8, HOP2):
            kept = hop.at[layer, kind]
            where(passes[kind], lambda: pltpu.make_async_copy(kept, kept, hop_send.at[layer, kind]).wait())


def finish(part_ref, rest_ref, gains, inner_t, outer_t, out_ref, rotated, made, sem):
    def copy(chunk, source, start):
        cols = pl.ds(chunk * CHUNK, CHUNK)
        return pltpu.make_async_copy(source.at[:, pl.ds(start, CHUNK)], out_ref.at[:, cols], sem.at[chunk])

    copies = [copy(chunk, part_ref, chunk * CHUNK) for chunk in range(CHUNKS) if chunk != LAST]
    for each in copies:
        each.start()
    for part in range(CHUNK // SUB):
        cols = pl.ds(part * SUB, SUB)
        rotated[...] = rest_ref[:, cols].astype(jnp.float32)
        made[:, cols] = blend(rotated, gains[1], inner_t[1], outer_t[1])
    copies.append(copy(LAST, made, 0))
    copies[-1].start()
    for each in copies:
        each.wait()


def per_device(stream_in, norm_gains, w_inner, w_outer):
    hbm = pl.BlockSpec(memory_space=pltpu.HBM)
    vmem = pl.BlockSpec(memory_space=pltpu.VMEM)
    kept = pl.pallas_call(
        body,
        out_shape=[
            pltpu.VMEM((DIM, COLS), jnp.bfloat16),
            pltpu.VMEM((DIM, CHUNK), jnp.bfloat16),
            pltpu.VMEM((LAYERS, DIM, LANES), jnp.float32),
            pltpu.VMEM((LAYERS, HID, DIM), jnp.bfloat16),
            pltpu.VMEM((LAYERS, DIM, HID), jnp.bfloat16),
        ],
        in_specs=[hbm, vmem, hbm, hbm],
        out_specs=[vmem] * 5,
        scratch_shapes=[
            pltpu.VMEM((LAYERS, NEAR_ROWS, PAD + COLS), jnp.bfloat16),
            pltpu.VMEM((LAYERS, FAR_ROWS, COLS), jnp.bfloat16),
            pltpu.VMEM((FAR_ROWS, COLS), jnp.bfloat16),
            pltpu.VMEM((LAYERS, 3, WIDTH, COLS), jnp.bfloat16),
            pltpu.VMEM((LAYERS, DIM, HID), jnp.bfloat16),
            pltpu.VMEM((DIM, SUB), jnp.float32),
            pltpu.SemaphoreType.DMA,
            pltpu.SemaphoreType.DMA((2,)),
            pltpu.SemaphoreType.DMA((LAYERS,)),
            pltpu.SemaphoreType.DMA((LAYERS, CHUNKS)),
            pltpu.SemaphoreType.DMA((LAYERS, 3)),
            pltpu.SemaphoreType.DMA((LAYERS, 3, CHUNKS)),
            pltpu.SemaphoreType.DMA((LAYERS, len(HALOS))),
            pltpu.SemaphoreType.DMA((LAYERS, len(HALOS))),
        ],
        compiler_params=pltpu.CompilerParams(
            collective_id=0, has_side_effects=True, vmem_limit_bytes=VMEM_BODY
        ),
        name="mix_and_send",
    )(stream_in, norm_gains, w_inner, jnp.swapaxes(w_outer, 1, 2))
    return pl.pallas_call(
        finish,
        out_shape=jax.ShapeDtypeStruct(stream_in.shape, stream_in.dtype),
        in_specs=[vmem] * 5,
        out_specs=hbm,
        scratch_shapes=[
            pltpu.VMEM((DIM, SUB), jnp.float32),
            pltpu.VMEM((DIM, CHUNK), jnp.bfloat16),
            pltpu.SemaphoreType.DMA((CHUNKS,)),
        ],
        compiler_params=pltpu.CompilerParams(vmem_limit_bytes=32 * 1024 * 1024),
        name="last_chunk_and_store",
    )(*kept)


def solution(mesh):
    return jax.shard_map(
        per_device,
        mesh=mesh,
        in_specs=(P(None, ("batch", "seq")), P(), P(), P()),
        out_specs=P(None, ("batch", "seq")),
        check_vma=False,
    )
```

```python
import functools

import jax
import jax.numpy as jnp
from jax import lax
from jax.experimental import pallas as pl
from jax.experimental.pallas import tpu as pltpu
from jax.sharding import PartitionSpec as P

TRACKS = 20
WIDTH = 16
LAYERS = 2
DIM = 320
HID = 640
RING = 128
COLS = 8192
NEAR = 13
NEAR_ROWS = NEAR * WIDTH
FAR_ROWS = DIM - NEAR_ROWS
PAD = 4096
CHUNKS = 8
CHUNK = COLS // CHUNKS
SUB = 1024
LANES = 128
LAST = CHUNKS // 2 - 1
VMEM_BODY = 57_000_000
FAR = tuple(2**e for e in range(TRACKS - NEAR))
HOP2, HOP8, HOP16 = range(3)
HOP_TRACK = (1, 3, 4)
WINDOW = 6
LEAD = 4
LAG = 4


def tails():
    pieces = [(0, 8 * WIDTH, LANES, CHUNKS - 1)]
    for track in range(8, NEAR):
        if 2**track < CHUNK:
            pieces.append((track * WIDTH, WIDTH, 2**track, CHUNKS - 1))
    for chunk in range(CHUNKS):
        need = [track for track in range(NEAR) if CHUNK <= 2**track and COLS - 2**track <= chunk * CHUNK]
        if need:
            pieces.append((need[0] * WIDTH, NEAR_ROWS - need[0] * WIDTH, CHUNK, chunk))
    return tuple(pieces)


HALOS = tails()


def halo_slices(index):
    row, rows, cols, chunk = HALOS[index]
    start = (chunk + 1) * CHUNK - cols
    return pl.ds(row, rows), start, cols


def blend(rotated, gain, inner_t, outer_t):
    values = rotated[...]
    average = jnp.sum(values, axis=0, keepdims=True) * (1.0 / DIM)
    centred = values - average
    spread = jnp.sum(centred * centred, axis=0, keepdims=True) * (1.0 / DIM)
    scale = lax.rsqrt(spread + 1e-05)
    gain = jnp.concatenate([gain] * (SUB // LANES), axis=1)
    normed = (centred * scale * gain).astype(jnp.bfloat16)
    inner_sum = jnp.dot(inner_t, normed, preferred_element_type=jnp.float32)
    hidden = (0.5 * inner_sum * (1.0 + lax.erf(inner_sum * (0.5**0.5)))).astype(jnp.bfloat16)
    outer_sum = jnp.dot(outer_t, hidden, preferred_element_type=jnp.float32)
    return (rotated[...] + outer_sum).astype(jnp.bfloat16)


def body(
    x_ref, gain_ref, inner_ref, outer_ref, out_ref, rest_ref, gains, inner_t, outer_t,
    near, far, made, hop, inner_raw, rotated,
    local_sem, weight_sem, far_send, far_recv, hop_send, hop_recv, halo_send, halo_recv,
):
    me = lax.axis_index("seq")
    row, depth = me // 32, lax.rem(me // 4, 8)
    half, core = lax.rem(me // 2, 2), lax.rem(me, 2)

    def device(y, z, x):
        return ((lax.rem(y + 4, 4) * 8 + lax.rem(z + 8, 8)) * 2 + x) * 2 + core

    ahead = [lax.rem(me + d, RING) for d in FAR]
    behind = [lax.rem(me + RING - d, RING) for d in FAR]
    deep = jnp.where(depth >= 4, 1, 0)
    last = jnp.where(depth == 7, 1, 0)
    hop_to = [
        device(row + last * half, depth, 1 - half),
        device(row + 1, depth, half),
        device(row + deep, depth - 2, half),
    ]
    hop_from = [
        device(row - last * (1 - half), depth, 1 - half),
        device(row - 1, depth, half),
        device(row - jnp.where(lax.rem(depth + 2, 8) >= 4, 1, 0), depth + 2, half),
    ]
    pass_to = [device(row, depth + 1, half), device(row, depth + 2, half), device(row, depth - 2, half)]
    pass_from = [device(row, depth - 1, half), device(row, depth - 2, half), device(row, depth + 2, half)]
    sends_hop = [half == 1, depth == 6, None]
    passes = [half == 0, depth == 6, None]

    def where(condition, action):
        if condition is None:
            action()
        else:
            pl.when(condition)(action)

    near_copy = pltpu.make_async_copy(
        x_ref.at[pl.ds(0, NEAR_ROWS), :], near.at[0, :, pl.ds(PAD, COLS)], local_sem
    )
    near_copy.start()
    inner_copy = pltpu.make_async_copy(inner_ref, inner_raw, weight_sem.at[0])
    outer_copy = pltpu.make_async_copy(outer_ref, outer_t, weight_sem.at[1])
    inner_copy.start()
    outer_copy.start()

    barrier = pltpu.get_barrier_semaphore()
    direct = [track for track in range(len(FAR)) if track != HOP_TRACK[HOP16]]
    peers = [ahead[track] for track in direct] + [behind[track] for track in direct]
    peers += hop_to + hop_from + pass_to + pass_from
    for peer in peers:
        pl.semaphore_signal(barrier, inc=1, device_id={"seq": peer})
    pl.semaphore_wait(barrier, len(peers))

    def halo_copy(layer, index, source):
        rows, start, cols = halo_slices(index)
        return pltpu.make_async_remote_copy(
            src_ref=source.at[rows, pl.ds(start + (0 if layer == 0 else PAD), cols)],
            dst_ref=near.at[layer, rows, pl.ds(start + PAD - COLS, cols)],
            send_sem=halo_send.at[layer, index],
            recv_sem=halo_recv.at[layer, index],
            device_id={"seq": ahead[0]},
        )

    def far_copy(layer, track, chunk, source, base):
        cols = pl.ds(pl.multiple_of(chunk * CHUNK, CHUNK), CHUNK)
        return pltpu.make_async_remote_copy(
            src_ref=source.at[pl.ds(base + track * WIDTH, WIDTH), cols],
            dst_ref=far.at[layer, pl.ds(track * WIDTH, WIDTH), cols],
            send_sem=far_send.at[layer],
            recv_sem=far_recv.at[layer, chunk],
            device_id={"seq": ahead[track]},
        )

    def hop_copy(layer, kind, chunk, source, base):
        cols = pl.ds(pl.multiple_of(chunk * CHUNK, CHUNK), CHUNK)
        return pltpu.make_async_remote_copy(
            src_ref=source.at[pl.ds(base + HOP_TRACK[kind] * WIDTH, WIDTH), cols],
            dst_ref=hop.at[layer, kind, :, cols],
            send_sem=far_send.at[layer],
            recv_sem=hop_recv.at[layer, kind, chunk],
            device_id={"seq": hop_to[kind]},
        )

    def pass_copy(layer, kind, chunk):
        cols = pl.ds(pl.multiple_of(chunk * CHUNK, CHUNK), CHUNK)
        return pltpu.make_async_remote_copy(
            src_ref=hop.at[layer, kind, :, cols],
            dst_ref=far.at[layer, pl.ds(HOP_TRACK[kind] * WIDTH, WIDTH), cols],
            send_sem=hop_send.at[layer, kind],
            recv_sem=far_recv.at[layer, chunk],
            device_id={"seq": pass_to[kind]},
        )

    def send_far(layer, chunk, source, base):
        for kind in (HOP16, HOP8, HOP2):
            where(sends_hop[kind], lambda: hop_copy(layer, kind, chunk, source, base).start())
        for track in range(len(FAR)):
            kind = HOP_TRACK.index(track) if track in HOP_TRACK else None
            if kind == HOP16:
                continue
            direct = None if kind is None else jnp.logical_not(sends_hop[kind])
            where(direct, lambda: far_copy(layer, track, chunk, source, base).start())

    def forward(layer, chunk):
        cols = pl.ds(pl.multiple_of(chunk * CHUNK, CHUNK), CHUNK)
        for kind in (HOP16, HOP8, HOP2):
            def relay():
                landed = hop.at[layer, kind, :, cols]
                pltpu.make_async_copy(landed, landed, hop_recv.at[layer, kind, chunk]).wait()
                pass_copy(layer, kind, chunk).start()

            where(passes[kind], relay)

    def turn(step):
        return lax.rem(step + CHUNKS // 2, CHUNKS)

    @pl.loop(0, 2)
    def _(step):
        send_far(0, turn(step), x_ref, NEAR_ROWS)

    for index in range(len(HALOS)):
        halo_copy(0, index, x_ref).start()

    @pl.loop(2, WINDOW)
    def _(step):
        send_far(0, turn(step), x_ref, NEAR_ROWS)

    for layer in range(LAYERS):
        gains[layer] = jnp.broadcast_to(gain_ref[layer : layer + 1, :], (LANES, DIM)).T
    inner_copy.wait()
    for layer in range(LAYERS):
        inner_t[layer] = inner_raw[layer].T
    outer_copy.wait()
    near_copy.wait()

    def gather_near(layer, at, keep):
        base = pl.multiple_of(PAD + at, LANES)
        for track in range(NEAR):
            shift = 2**track
            rows = pl.ds(track * WIDTH, WIDTH)
            if shift < LANES:
                wide = near[layer, rows, pl.ds(pl.multiple_of(base - LANES, LANES), SUB + LANES)]
                piece = pltpu.roll(wide.astype(jnp.float32), shift, 1)[:, LANES:]
            else:
                piece = near[layer, rows, pl.ds(pl.multiple_of(base - shift, LANES), SUB)].astype(jnp.float32)
            keep(rows, piece)

    def mix(layer, at, store):
        def keep(rows, piece):
            rotated[rows, :] = piece

        gather_near(layer, at, keep)
        rotated[NEAR_ROWS:, :] = far[layer, :, pl.ds(pl.multiple_of(at, LANES), SUB)].astype(jnp.float32)
        store(blend(rotated, gains[layer], inner_t[layer], outer_t[layer]))

    def wait_far(layer, chunk):
        cols = pl.ds(pl.multiple_of(chunk * CHUNK, CHUNK), CHUNK)
        whole = far.at[layer, :, cols]
        pltpu.make_async_copy(whole, whole, far_recv.at[layer, chunk]).wait()

    def wait_halos(layer, source):
        for index in range(len(HALOS)):
            halo_copy(layer, index, source).wait_recv()

    for step in range(LEAD):
        forward(0, turn(step))

    @pl.loop(0, CHUNKS)
    def _(step):
        chunk = turn(step)

        @pl.when(step < CHUNKS - WINDOW)
        def _():
            send_far(0, turn(step + WINDOW), x_ref, NEAR_ROWS)

        @pl.when(step < CHUNKS - LEAD)
        def _():
            forward(0, turn(step + LEAD))

        @pl.when(step >= LAG)
        def _():
            forward(1, turn(step - LAG))

        wait_far(0, chunk)

        @pl.when(step == CHUNKS // 2)
        def _():
            wait_halos(0, x_ref)

        @pl.loop(0, CHUNK // SUB)
        def _(part):
            at = pl.multiple_of(chunk * CHUNK + part * SUB, SUB)

            def store(result):
                near[1, :, pl.ds(pl.multiple_of(PAD + at, SUB), SUB)] = result[:NEAR_ROWS]
                made[:, pl.ds(at, SUB)] = result[NEAR_ROWS:]

            mix(0, at, store)

        send_far(1, chunk, made, 0)
        for index, halo in enumerate(HALOS):
            @pl.when(chunk == halo[3])
            def _():
                halo_copy(1, index, near.at[1]).start()

    @pl.loop(0, CHUNKS - 1)
    def _(step):
        chunk = lax.rem(step + CHUNKS // 2, CHUNKS)

        @pl.when(step < LAG)
        def _():
            forward(1, turn(step + CHUNKS - LAG))

        wait_far(1, chunk)

        @pl.when(step == CHUNKS // 2)
        def _():
            wait_halos(1, near.at[1])

        @pl.loop(0, CHUNK // SUB)
        def _(part):
            at = pl.multiple_of(chunk * CHUNK + part * SUB, SUB)

            def store(result):
                out_ref[:, pl.ds(at, SUB)] = result

            mix(1, at, store)

    for part in range(CHUNK // SUB):
        cols = pl.ds(part * SUB, SUB)

        def keep(rows, piece):
            rest_ref[rows, cols] = piece.astype(jnp.bfloat16)

        gather_near(1, LAST * CHUNK + part * SUB, keep)

    wait_far(1, LAST)
    rest_ref[NEAR_ROWS:, :] = far[1, :, pl.ds(LAST * CHUNK, CHUNK)]
    for layer in range(LAYERS):
        source = x_ref if layer == 0 else near.at[1]
        for index in range(len(HALOS)):
            halo_copy(layer, index, source).wait_send()
        pltpu.make_async_copy(far.at[layer], far.at[layer], far_send.at[layer]).wait()
        for kind in (HOP16, HOP8, HOP2):
            kept = hop.at[layer, kind]
            where(passes[kind], lambda: pltpu.make_async_copy(kept, kept, hop_send.at[layer, kind]).wait())


def finish(part_ref, rest_ref, gains, inner_t, outer_t, out_ref, rotated, made, sem):
    def copy(chunk, source, start):
        cols = pl.ds(chunk * CHUNK, CHUNK)
        return pltpu.make_async_copy(source.at[:, pl.ds(start, CHUNK)], out_ref.at[:, cols], sem.at[chunk])

    copies = [copy(chunk, part_ref, chunk * CHUNK) for chunk in range(CHUNKS) if chunk != LAST]
    for each in copies:
        each.start()
    for part in range(CHUNK // SUB):
        cols = pl.ds(part * SUB, SUB)
        rotated[...] = rest_ref[:, cols].astype(jnp.float32)
        made[:, cols] = blend(rotated, gains[1], inner_t[1], outer_t[1])
    copies.append(copy(LAST, made, 0))
    copies[-1].start()
    for each in copies:
        each.wait()


def per_device(stream_in, norm_gains, w_inner, w_outer):
    hbm = pl.BlockSpec(memory_space=pltpu.HBM)
    vmem = pl.BlockSpec(memory_space=pltpu.VMEM)
    kept = pl.pallas_call(
        body,
        out_shape=[
            pltpu.VMEM((DIM, COLS), jnp.bfloat16),
            pltpu.VMEM((DIM, CHUNK), jnp.bfloat16),
            pltpu.VMEM((LAYERS, DIM, LANES), jnp.float32),
            pltpu.VMEM((LAYERS, HID, DIM), jnp.bfloat16),
            pltpu.VMEM((LAYERS, DIM, HID), jnp.bfloat16),
        ],
        in_specs=[hbm, vmem, hbm, hbm],
        out_specs=[vmem] * 5,
        scratch_shapes=[
            pltpu.VMEM((LAYERS, NEAR_ROWS, PAD + COLS), jnp.bfloat16),
            pltpu.VMEM((LAYERS, FAR_ROWS, COLS), jnp.bfloat16),
            pltpu.VMEM((FAR_ROWS, COLS), jnp.bfloat16),
            pltpu.VMEM((LAYERS, 3, WIDTH, COLS), jnp.bfloat16),
            pltpu.VMEM((LAYERS, DIM, HID), jnp.bfloat16),
            pltpu.VMEM((DIM, SUB), jnp.float32),
            pltpu.SemaphoreType.DMA,
            pltpu.SemaphoreType.DMA((2,)),
            pltpu.SemaphoreType.DMA((LAYERS,)),
            pltpu.SemaphoreType.DMA((LAYERS, CHUNKS)),
            pltpu.SemaphoreType.DMA((LAYERS, 3)),
            pltpu.SemaphoreType.DMA((LAYERS, 3, CHUNKS)),
            pltpu.SemaphoreType.DMA((LAYERS, len(HALOS))),
            pltpu.SemaphoreType.DMA((LAYERS, len(HALOS))),
        ],
        compiler_params=pltpu.CompilerParams(
            collective_id=0, has_side_effects=True, vmem_limit_bytes=VMEM_BODY
        ),
        name="mix_and_send",
    )(stream_in, norm_gains, w_inner, jnp.swapaxes(w_outer, 1, 2))
    return pl.pallas_call(
        finish,
        out_shape=jax.ShapeDtypeStruct(stream_in.shape, stream_in.dtype),
        in_specs=[vmem] * 5,
        out_specs=hbm,
        scratch_shapes=[
            pltpu.VMEM((DIM, SUB), jnp.float32),
            pltpu.VMEM((DIM, CHUNK), jnp.bfloat16),
            pltpu.SemaphoreType.DMA((CHUNKS,)),
        ],
        compiler_params=pltpu.CompilerParams(vmem_limit_bytes=32 * 1024 * 1024),
        name="last_chunk_and_store",
    )(*kept)


def solution(mesh):
    return jax.shard_map(
        per_device,
        mesh=mesh,
        in_specs=(P(None, ("batch", "seq")), P(), P(), P()),
        out_specs=P(None, ("batch", "seq")),
        check_vma=False,
    )
```
